32 devices in a mesh: gx: 8 (over z, x), gy: 4 (over y, core).
Axes of the slice: x: 2, y: 2, z: 4, core: 2. Of those that a mesh axis runs over, the one named last changes fastest.
Arguments:
- pooled: bfloat16 [4096, 8, 128], P(('gx', 'gy')), may hold values from -6 to 6
- cotangent: bfloat16 [4096, 28, 128], P(('gx', 'gy')), may hold values from -0.09375 to 0.09375
- bilinear: bfloat16 [7, 128, 128], replicated, may hold values from -0.5 to 0.5
- bag_ids: int32 [4096, 8, 4], P(('gx', 'gy')), may hold values from 0 to 8191, as said below
- bag_lens: int32 [4096, 8], P(('gx', 'gy')), may hold values from 1 to 4
- row_home: int32 [8, 8192], replicated, may hold values from 0 to 8191, as said below
Outputs:
- weight_grad: float32 [7, 128, 128], replicated
- table_grad: float32 [8192, 8, 128], P(('gx', 'gy'))
The draws below stay inside these ranges and needn't reach their ends.
Inputs may be any that keep to these rules, and one draw needn't show every extreme that they name: Each row row_home[f] is a permutation; row r of field f's table is stored at position row_home[f, r] of table_grad's first dimension. Only the first bag_lens entries of a bag are live. The stored position q = row_home[f, bag_ids[sample, f, k]] of an entry lies in the block of 256 positions of device q // 256 (devices in gx+gy order); among all entries of one device's samples, live or not, at most 256 lie in any one device's block; in every device's entries some block is hit exactly 256 times, and one block is hit exactly 256 times by the entries of every device.
All inputs are finite; a program needn't handle non-finite values.
Results may differ from the reference program's by a relative error of at most 0.0035.
Values may be sent and summed in bfloat16 or wider, within the bound.
A program may use at most 64 MiB of HBM per device.

```python
import jax
import jax.numpy as jnp
from jax import lax

D = 128
FIELDS = 8
PAIRS = 28
BAG = 4
TOK_DEV = 128
R_DEV = 256
TOKENS = 4096
ROWS = 8192
CAP = 256
N_GX = 8
N_GY = 4


def home_table(key):
    field_keys = jax.random.split(jax.random.fold_in(key, 101), FIELDS)
    return jax.vmap(lambda k: jax.random.permutation(k, ROWS))(field_keys).astype(jnp.int32)


def draw_row_home(key, part):
    return home_table(key)


def draw_bag_ids(key, part):
    home = home_table(key)
    inverse = jnp.argsort(home, axis=1, stable=True).astype(jnp.int32)
    owners_all = N_GX * N_GY
    slots = CAP * owners_all
    entries = TOK_DEV * FIELDS * BAG
    route_key = jax.random.fold_in(key, 202)
    hotness = jax.random.randint(jax.random.fold_in(route_key, 1), (owners_all,), 0, 4).astype(jnp.int32)
    shared_full = jax.random.randint(jax.random.fold_in(route_key, 2), (), 0, owners_all).astype(jnp.int32)
    slot_owner = (jnp.arange(slots, dtype=jnp.int32) // CAP).astype(jnp.int32)

    def one_block(block):
        block_key = jax.random.fold_in(route_key, 1000 + block)
        raw = jax.random.randint(jax.random.fold_in(block_key, 1), (slots,), 0, 4096).astype(jnp.int32)
        score = jnp.right_shift(raw, 2 * hotness[slot_owner])
        own_full = jax.random.randint(jax.random.fold_in(block_key, 2), (), 0, owners_all).astype(jnp.int32)
        forced = jnp.logical_or(slot_owner == own_full, slot_owner == shared_full)
        score = jnp.where(forced, -1, score)
        rank_key = score * slots + jnp.arange(slots, dtype=jnp.int32)
        picked = jnp.argsort(rank_key, stable=True)[:entries]
        owners = slot_owner[picked]
        owners = owners[jax.random.permutation(jax.random.fold_in(block_key, 3), entries)]
        first = jax.random.randint(jax.random.fold_in(block_key, 4), (entries,), 0, R_DEV).astype(jnp.int32)
        second = jax.random.randint(jax.random.fold_in(block_key, 5), (entries,), 0, R_DEV).astype(jnp.int32)
        local = first * second // R_DEV
        return (owners * R_DEV + local).astype(jnp.int32)
    stored = lax.map(one_block, jnp.arange(owners_all, dtype=jnp.int32)).reshape(TOKENS, FIELDS, BAG)
    field_index = jnp.arange(FIELDS, dtype=jnp.int32)[None, :, None]
    return inverse[field_index, stored].astype(jnp.int32)


def plant(result, key, low, high):
    spot = [jax.random.randint(jax.random.fold_in(key, axis), (), 0, length) for axis, length in enumerate(result.shape)]
    widest = result.shape.index(max(result.shape))
    beside = spot[:widest] + [(spot[widest] + 1) % result.shape[widest]] + spot[widest + 1:]
    return result.at[tuple(spot)].set(low).at[tuple(beside)].set(high)


def steps_of(stream_key, extent, cuts, smallest, largest):
    gain = 1.0
    for axis_at, blocks in cuts:
        draws = jax.random.uniform(jax.random.fold_in(jax.random.fold_in(stream_key, 6), axis_at), (blocks,), jnp.float32, smallest / len(cuts), largest / len(cuts))
        gain = gain * jnp.repeat(jnp.exp(draws), extent[axis_at] // blocks).reshape((-1,) + (1,) * (len(extent) - 1 - axis_at))
    return gain


def scatter_about(key, shape, width, most, shards=(), held_as=jnp.bfloat16):
    level = steps_of(key, shape, shards, -0.22, 0.18) if shards else 1.0
    result = jax.random.normal(key, shape, jnp.float32) * width * level
    return jnp.minimum(jnp.maximum(result, -most), most).astype(held_as)


def setup_inputs(seed: int = 0) -> dict:
    key_of = jax.random.split(jax.random.key(seed), 7)
    return {
        "pooled": scatter_about(key_of[0], (TOKENS, FIELDS, D), 1.0, 6.0, ((0, 32),)),
        "cotangent": scatter_about(key_of[1], (TOKENS, PAIRS, D), TOKENS ** -0.5, 0.09375, ((0, 32),)),
        "bilinear": scatter_about(key_of[2], (FIELDS - 1, D, D), D ** -0.5, 0.5),
        "bag_ids": draw_bag_ids(jax.random.fold_in(key_of[6], 71), 0),
        "bag_lens": plant(jax.random.randint(key_of[4], (TOKENS, FIELDS), 1, BAG + 1), jax.random.fold_in(key_of[4], 1), 1, BAG).astype(jnp.int32),
        "row_home": draw_row_home(jax.random.fold_in(key_of[6], 71), 0),
    }


def pair_list(fields):
    return [(i, j) for i in range(fields) for j in range(i + 1, fields)]


def reference(pooled, cotangent, bilinear, bag_ids, bag_lens, row_home):
    pair_order = pair_list(FIELDS)
    embedded = pooled.astype(jnp.float32)
    weights = bilinear.astype(jnp.float32)
    cot_rows = cotangent.astype(jnp.float32)
    projected = jnp.einsum('bfd,fde->bfe', embedded[:, :FIELDS - 1], weights)
    upper_terms = []
    for i in range(FIELDS - 1):
        running = jnp.zeros((TOKENS, D), jnp.float32)
        for p, (a, c) in enumerate(pair_order):
            if a == i:
                running = running + cot_rows[:, p] * embedded[:, c]
        upper_terms.append(running)
    upper_bf = jnp.stack(upper_terms, 1).astype(jnp.bfloat16).astype(jnp.float32)
    weight_grad = jnp.einsum('bfd,bfe->fde', embedded[:, :FIELDS - 1], upper_bf)
    field_list = []
    for i in range(FIELDS):
        running = jnp.zeros((TOKENS, D), jnp.float32)
        if i < FIELDS - 1:
            running = running + jnp.einsum('be,de->bd', upper_bf[:, i], weights[i])
        for p, (a, c) in enumerate(pair_order):
            if c == i:
                running = running + cot_rows[:, p] * projected[:, a]
        field_list.append(running)
    field_grads = jnp.stack(field_list, 1).astype(jnp.bfloat16).astype(jnp.float32)
    live = jnp.arange(BAG, dtype=jnp.int32)[None, :]
    tables = []
    for f in range(FIELDS):
        stored = row_home[f][bag_ids[:, f, :]]
        segment = jnp.where(live < bag_lens[:, f, None], stored, ROWS).astype(jnp.int32)
        values = jnp.broadcast_to(field_grads[:, f, None, :], (TOKENS, BAG, D)).reshape(TOKENS * BAG, D)
        summed = jax.ops.segment_sum(values, segment.reshape(-1), num_segments=ROWS + 1)
        tables.append(summed[:ROWS])
    return weight_grad, jnp.stack(tables, 1)
```

```python
import functools

import jax
import jax.numpy as jnp
from jax import lax
from jax.experimental import pallas as pl
from jax.experimental.pallas import tpu as pltpu
from jax.sharding import PartitionSpec as P

MESH = pl.DeviceIdType.MESH
BF = jnp.bfloat16
F32 = jnp.float32
LANES = 128


def pair_list(fields):
    return [(i, j) for i in range(fields) for j in range(i + 1, fields)]


def local_kernel(
    pooled_ref, cot_ref, bil_ref, bag_ref, lens_ref, home_ref,
    grad_ref, weight_ref, ids_ref, pool_f, cot_f, proj_f,
):
    samples, fields, width = pooled_ref.shape
    pairs = cot_ref.shape[1]
    stride = cot_f.shape[0] // samples
    bag = bag_ref.shape[0]

    def spread(b, carry):
        pool_f[pl.ds(pl.multiple_of(b * fields, fields), fields), :] = pooled_ref[b].astype(F32)
        cot_f[pl.ds(pl.multiple_of(b * stride, stride), pairs), :] = cot_ref[b].astype(F32)
        return carry

    lax.fori_loop(0, samples, spread, 0, unroll=8)

    high = [bag_ref[k] // LANES for k in range(bag)]
    low = [bag_ref[k] % LANES for k in range(bag)]

    def look(h, found):
        row = home_ref[:, pl.ds(pl.multiple_of(h * LANES, LANES), LANES)]
        return tuple(
            jnp.where(high[k] == h, jnp.take_along_axis(row, low[k], axis=1), found[k])
            for k in range(bag)
        )

    none = jnp.full(bag_ref.shape[1:], -1, jnp.int32)
    found = lax.fori_loop(0, home_ref.shape[1] // LANES, look, (none,) * bag, unroll=8)
    lens = lens_ref[...]
    for k in range(bag):
        ids_ref[k] = jnp.where(lens > k, found[k], -1)

    pool = lambda f: pool_f[pl.ds(f, samples, stride=fields), :]
    cot = lambda p: cot_f[pl.ds(p, samples, stride=stride), :]
    number = {pair: p for p, pair in enumerate(pair_list(fields))}
    for i in range(fields - 1):
        proj_f[i] = jnp.dot(pool(i).astype(BF), bil_ref[i], preferred_element_type=F32)
    for i in range(fields):
        total = jnp.zeros((samples, width), F32)
        if i < fields - 1:
            upper = jnp.zeros((samples, width), F32)
            for j in range(i + 1, fields):
                upper = upper + cot(number[i, j]) * pool(j)
            upper = upper.astype(BF)
            weight_ref[i] = lax.dot_general(
                pool(i).astype(BF), upper, (((0,), (0,)), ((), ())), preferred_element_type=F32
            ).astype(BF)
            total = lax.dot_general(
                upper, bil_ref[i], (((1,), (1,)), ((), ())), preferred_element_type=F32
            )
        for k in range(i):
            total = total + cot(number[k, i]) * proj_f[k]
        grad_ref[i] = total.astype(BF)


def exchange_kernel(
    size_gx, size_gy,
    grad_ref, ids_ref, w_ref, out_ref, wout_ref,
    gath, idg, part, got, w1, w2, w2s, w3, w3s,
    zs, zr, ss, sr, ps, pr, w1s_sem, w1r_sem, w2s_sem, w2r_sem, w3s_sem, w3r_sem,
):
    fields, samples, width = grad_ref.shape
    bag = ids_ref.shape[0]
    rows = part.shape[2]
    nz, ny = size_gx // 2, size_gy // 2
    npc, plane = 2 * ny, 2 * size_gy
    gx, gy = lax.axis_index("gx"), lax.axis_index("gy")
    z, x, y, c = gx // 2, gx % 2, gy // 2, gy % 2
    spot = x * ny + y
    seat = x * size_gy + gy
    sibling = (gx, y * 2 + 1 - c)

    def z_peer(d):
        return (((z + d) % nz) * 2 + x, gy)

    def spot_peer(d):
        to = (spot + d) % npc
        return (z * 2 + to // ny, (to % ny) * 2 + c)

    def seat_peer(d):
        to = (seat + d) % plane
        return (z * 2 + to // size_gy, to % size_gy)

    def remote(src, dst, send, recv, dev):
        return pltpu.make_async_remote_copy(
            src_ref=src, dst_ref=dst, send_sem=send, recv_sem=recv,
            device_id=dev, device_id_type=MESH,
        )

    def z_copy(f, d):
        return remote(grad_ref.at[f], gath.at[f, d], zs.at[f * nz + d], zr.at[f * nz + d], z_peer(d))

    def z_ids(d):
        return remote(ids_ref, idg.at[d], zs.at[fields * nz + d], zr.at[fields * nz + d], z_peer(d))

    def s_copy(f, d):
        src = grad_ref.at[f] if d == 0 else gath.at[f, d]
        return remote(src, gath.at[f, nz + d], ss.at[f * nz + d], sr.at[f * nz + d], sibling)

    def s_ids(d):
        src = ids_ref if d == 0 else idg.at[d]
        return remote(src, idg.at[nz + d], ss.at[fields * nz + d], sr.at[fields * nz + d], sibling)

    def p_copy(f, d):
        return remote(part.at[d, f], got.at[d, f], ps.at[f * npc + d], pr.at[f * npc + d], spot_peer(d))

    def w1_copy(d):
        return remote(
            w_ref.at[(seat + d) % plane], w1.at[d], w1s_sem.at[d], w1r_sem.at[d], seat_peer(d)
        )

    def w2_copy(d, slot):
        return remote(w2s, w2.at[slot], w2s_sem.at[d], w2r_sem.at[slot], z_peer(d))

    def w3_copy(d, slot):
        return remote(w3s, w3.at[slot], w3s_sem.at[d], w3r_sem.at[slot], seat_peer(d))

    barrier = pltpu.get_barrier_semaphore()
    for d in range(1, nz):
        pl.semaphore_signal(barrier, inc=1, device_id=z_peer(d), device_id_type=MESH)
    for d in range(1, plane):
        pl.semaphore_signal(barrier, inc=1, device_id=seat_peer(d), device_id_type=MESH)
    pl.semaphore_wait(barrier, nz - 1 + plane - 1)

    for d in range(1, nz):
        z_ids(d).start()
    s_ids(0).start()

    def launch(f, carry):
        for d in range(1, nz):
            z_copy(f, d).start()
        s_copy(f, 0).start()
        return carry

    lax.fori_loop(0, fields, launch, 0)
    for d in range(1, plane):
        w1_copy(d).start()
    gath[:, 0] = grad_ref[...]
    idg[0] = ids_ref[...]

    def forward(f):
        for d in range(1, nz):
            z_copy(f, d).wait_recv()
            s_copy(f, d).start()

    for d in range(1, nz):
        z_ids(d).wait_recv()
        s_ids(d).start()
    forward(0)
    for d in range(nz):
        s_ids(d).wait_recv()

    kind = BF if rows <= 256 else F32
    row_number = lax.broadcasted_iota(jnp.int32, (rows, samples), 0).astype(F32).astype(kind)
    one, zero = jnp.ones((), kind), jnp.zeros((), kind)

    def sums_for(f, d):
        gx_to, gy_to = spot_peer(d)
        base = (gx_to * size_gy + gy_to) * rows
        blocks = []
        for j in range(2 * nz):
            count = None
            for k in range(bag):
                rel = idg[j, k, pl.ds(f, 1), :] - base
                rel = jnp.where((rel >= 0) & (rel < rows), rel, rows).astype(F32).astype(kind)
                hit = jnp.where(row_number == rel, one, zero)
                count = hit if count is None else count + hit
            blocks.append(count.astype(BF))
        return jnp.dot(
            jnp.concatenate(blocks, axis=1),
            gath[f].reshape(2 * nz * samples, width),
            preferred_element_type=F32,
        )

    def weights_in_plane():
        total = w_ref[seat].astype(F32)
        for d in range(1, plane):
            w1_copy(d).wait_recv()
            total = total + w1[d].astype(F32)
        w2s[...] = total.astype(BF)
        w2[z] = total.astype(BF)
        for d in range(1, nz):
            w2_copy(d, z).start()

    def weights_along_z():
        for d in range(1, nz):
            w2_copy(d, (z + d) % nz).wait_recv()
        total = w2[0].astype(F32)
        for s in range(1, nz):
            total = total + w2[s].astype(F32)
        w3s[...] = total.astype(BF)
        w3[seat] = total.astype(BF)
        for d in range(1, plane):
            w3_copy(d, seat).start()

    def one_field(f, carry):
        @pl.when(f + 1 < fields)
        def _():
            forward(f + 1)

        for d in range(nz):
            s_copy(f, d).wait_recv()

        def one_target(d, inner):
            part[d, f] = sums_for(f, d).astype(BF)
            p_copy(f, d).start()
            return inner

        lax.fori_loop(1, npc, one_target, 0)
        out_ref[pl.ds(f, rows, stride=fields), :] = sums_for(f, 0)

        @pl.when(f == 1)
        def _():
            weights_in_plane()

        @pl.when(f == 4)
        def _():
            weights_along_z()

        return carry

    lax.fori_loop(0, fields, one_field, 0)

    for d in range(1, plane):
        w3_copy(d, (seat + d) % plane).wait_recv()
    wout_ref[...] = w3[...].astype(F32)

    def finish(f, carry):
        at = pl.ds(f, rows, stride=fields)
        total = out_ref[at, :]
        for d in range(1, npc):
            p_copy(f, d).wait_recv()
            total = total + got[d, f].astype(F32)
        out_ref[at, :] = total
        return carry

    lax.fori_loop(0, fields, finish, 0)

    def drain(f, carry):
        for d in range(1, nz):
            z_copy(f, d).wait_send()
        for d in range(nz):
            s_copy(f, d).wait_send()
        for d in range(1, npc):
            p_copy(f, d).wait_send()
        return carry

    lax.fori_loop(0, fields, drain, 0)
    for d in range(1, nz):
        z_ids(d).wait_send()
        w2_copy(d, z).wait_send()
    for d in range(nz):
        s_ids(d).wait_send()
    for d in range(1, plane):
        w1_copy(d).wait_send()
        w3_copy(d, seat).wait_send()


def on_device(size_gx, size_gy, pooled, cotangent, bilinear, bag_ids, bag_lens, row_home):
    samples, fields, width = pooled.shape
    bag = bag_ids.shape[2]
    pairs = cotangent.shape[1]
    devices = size_gx * size_gy
    rows = row_home.shape[1] // devices
    nz, npc, plane = size_gx // 2, size_gy, 2 * size_gy
    stride = -(-pairs // 8) * 8
    vmem = pl.BlockSpec(memory_space=pltpu.VMEM)
    grads, weights, ids = pl.pallas_call(
        local_kernel,
        out_shape=(
            jax.ShapeDtypeStruct((fields, samples, width), BF),
            jax.ShapeDtypeStruct((fields - 1, width, width), BF),
            jax.ShapeDtypeStruct((bag, fields, samples), jnp.int32),
        ),
        in_specs=[vmem] * 6,
        out_specs=(vmem,) * 3,
        scratch_shapes=[
            pltpu.VMEM((samples * fields, width), F32),
            pltpu.VMEM((samples * stride, width), F32),
            pltpu.VMEM((fields - 1, samples, width), F32),
        ],
    )(
        pooled, cotangent, bilinear,
        bag_ids.transpose(2, 1, 0), bag_lens.transpose(1, 0), row_home,
    )
    piece = (fields - 1) * width // plane
    dma = pltpu.SemaphoreType.DMA
    table, weight = pl.pallas_call(
        functools.partial(exchange_kernel, size_gx, size_gy),
        out_shape=(
            jax.ShapeDtypeStruct((rows * fields, width), F32),
            jax.ShapeDtypeStruct((plane, piece, width), F32),
        ),
        in_specs=[vmem] * 3,
        out_specs=(vmem,) * 2,
        scratch_shapes=[
            pltpu.VMEM((fields, 2 * nz, samples, width), BF),
            pltpu.VMEM((2 * nz, bag, fields, samples), jnp.int32),
            pltpu.VMEM((npc, fields, rows, width), BF),
            pltpu.VMEM((npc, fields, rows, width), BF),
            pltpu.VMEM((plane, piece, width), BF),
            pltpu.VMEM((nz, piece, width), BF),
            pltpu.VMEM((piece, width), BF),
            pltpu.VMEM((plane, piece, width), BF),
            pltpu.VMEM((piece, width), BF),
            dma(((fields + 1) * nz,)),
            dma(((fields + 1) * nz,)),
            dma(((fields + 1) * nz,)),
            dma(((fields + 1) * nz,)),
            dma((fields * npc,)),
            dma((fields * npc,)),
            dma((plane,)),
            dma((plane,)),
            dma((nz,)),
            dma((nz,)),
            dma((plane,)),
            dma((plane,)),
        ],
        compiler_params=pltpu.CompilerParams(collective_id=0, has_side_effects=True),
    )(grads, ids, weights.reshape(plane, piece, width))
    return (
        weight.reshape(fields - 1, width, width),
        table.reshape(rows, fields, width),
    )


def solution(mesh):
    placed = (
        P(("gx", "gy"), None, None),
        P(("gx", "gy"), None, None),
        P(),
        P(("gx", "gy"), None, None),
        P(("gx", "gy"), None),
        P(),
    )
    return jax.shard_map(
        functools.partial(on_device, mesh.shape["gx"], mesh.shape["gy"]),
        mesh=mesh,
        in_specs=placed,
        out_specs=(P(), P(("gx", "gy"), None, None)),
        check_vma=False,
    )
```

```python
import functools

import jax
import jax.numpy as jnp
from jax import lax
from jax.experimental import pallas as pl
from jax.experimental.pallas import tpu as pltpu
from jax.sharding import PartitionSpec as P

MESH = pl.DeviceIdType.MESH
BF = jnp.bfloat16
F32 = jnp.float32
LANES = 128


def pair_list(fields):
    return [(i, j) for i in range(fields) for j in range(i + 1, fields)]


def kernel(
    size_gx, size_gy,
    pooled_ref, cot_ref, bil_ref, bag_ref, lens_ref, home_ref,
    out_ref, wout_ref,
    pool_f, proj_f, meta,
    gath0, gath1, part0, part1, got0, got1,
    w0, w1, w2, w2s, w3, w3s,
    zus, zds, zr, as_, ar, ss, sr, ps, pr,
    w1s_sem, w1r_sem, w2s_sem, w2r_sem, w3s_sem, w3r_sem,
):
    samples, fields, width = pooled_ref.shape
    bag = bag_ref.shape[1]
    rows = part0.shape[2]
    piece = w0.shape[1]
    nz, ny = size_gx // 2, size_gy // 2
    plane = 2 * size_gy
    most = max(2, ny)
    gx, gy = lax.axis_index("gx"), lax.axis_index("gy")
    z, x, y, c = gx // 2, gx % 2, gy // 2, gy % 2
    seat = x * size_gy + gy
    sibling = (gx, y * 2 + 1 - c)
    gath, part, got = (gath0, gath1), (part0, part1), (got0, got1)
    wide, deep = (2, ny), (ny, 2)

    def along_x(o):
        return (z * 2 + (x + o) % 2, gy)

    def along_y(o):
        return (gx, ((y + o) % ny) * 2 + c)

    near, far = (along_x, along_y), (along_y, along_x)

    def z_peer(d):
        return (((z + d) % nz) * 2 + x, gy)

    def seat_peer(d):
        to = (seat + d) % plane
        return (z * 2 + to // size_gy, to % size_gy)

    def remote(src, dst, send, recv, dev):
        return pltpu.make_async_remote_copy(
            src_ref=src, dst_ref=dst, send_sem=send, recv_sem=recv,
            device_id=dev, device_id_type=MESH,
        )

    def z_up(g, m, s):
        slot, i = gath[m].at[g, 0, 0, s], (2 * g + m) * nz + s
        return remote(slot, slot, zus.at[i], zr.at[i], z_peer(1))

    def z_down(g, m, s):
        slot, i = gath[m].at[g, 0, 0, s], (2 * g + m) * nz + s
        return remote(slot, slot, zds.at[i], zr.at[i], z_peer(nz - 1))

    def a_copy(g, m, o, s):
        i = ((2 * g + m) * most + o) * nz + s
        return remote(
            gath[m].at[g, 0, 0, s], gath[m].at[g, 0, o, s], as_.at[i], ar.at[i], near[m](o)
        )

    def s_copy(g, m, o, s):
        i = ((2 * g + m) * most + o) * nz + s
        return remote(
            gath[m].at[g, 0, o, s], gath[m].at[g, 1, o, s], ss.at[i], sr.at[i], sibling
        )

    def p_copy(g, m, o):
        i = (2 * g + m) * most + o
        return remote(part[m].at[o, g], got[m].at[o, g], ps.at[i], pr.at[i], far[m](o))

    def w1_copy(d):
        return remote(
            w0.at[(seat + d) % plane], w1.at[d], w1s_sem.at[d], w1r_sem.at[d], seat_peer(d)
        )

    def w2_copy(d, slot):
        return remote(w2s, w2.at[slot], w2s_sem.at[d], w2r_sem.at[slot], z_peer(d))

    def w3_copy(d, slot):
        return remote(w3s, w3.at[slot], w3s_sem.at[d], w3r_sem.at[slot], seat_peer(d))

    barrier = pltpu.get_barrier_semaphore()
    for d in range(1, nz):
        pl.semaphore_signal(barrier, inc=1, device_id=z_peer(d), device_id_type=MESH)
    for d in range(1, plane):
        pl.semaphore_signal(barrier, inc=1, device_id=seat_peer(d), device_id_type=MESH)

    def spread_out(b, carry):
        pool_f[pl.ds(pl.multiple_of(b * fields, fields), fields), :] = pooled_ref[b].astype(F32)
        return carry

    lax.fori_loop(0, samples, spread_out, 0, unroll=8)

    bags = [bag_ref[:, k, :] for k in range(bag)]
    high = [b // LANES for b in bags]
    low = [b % LANES for b in bags]

    def look(h, found):
        row = home_ref[:, pl.ds(pl.multiple_of(h * LANES, LANES), LANES)]
        return tuple(
            jnp.where(high[k] == h, jnp.take_along_axis(row, low[k], axis=1), found[k])
            for k in range(bag)
        )

    none = jnp.full(lens_ref.shape, 0, jnp.int32)
    found = lax.fori_loop(0, home_ref.shape[1] // LANES, look, (none,) * bag, unroll=8)
    lens = lens_ref[...]
    for k in range(bag):
        meta[:, k, :] = jnp.where(lens > k, found[k] // rows, -1).astype(F32)
        meta[:, bag + k, :] = (found[k] % rows).astype(F32)

    pool = lambda f: pool_f[pl.ds(f, samples, stride=fields), :]
    number = {pair: p for p, pair in enumerate(pair_list(fields))}
    cot = lambda i, j: cot_ref[number[i, j]].astype(F32)

    def spread(g, m, s):
        for o in range(1, wide[m]):
            a_copy(g, m, o, s).start()
        s_copy(g, m, 0, s).start()

    for i in range(fields):
        total = None
        if i < fields - 1:
            mine = pool(i).astype(BF)
            proj_f[i] = jnp.dot(mine, bil_ref[i], preferred_element_type=F32)
            upper = jnp.zeros((samples, width), F32)
            for j in range(i + 1, fields):
                upper = upper + cot(i, j) * pool(j)
            upper = upper.astype(BF)
            wide_w = lax.dot_general(
                mine, upper, (((0,), (0,)), ((), ())), preferred_element_type=F32
            ).astype(BF)
            at, end = i * width, (i + 1) * width
            while at < end:
                p, r = at // piece, at % piece
                n = min(piece - r, end - at)
                w0[p, r : r + n, :] = wide_w[at - i * width : at - i * width + n, :]
                at += n
            total = lax.dot_general(
                upper, bil_ref[i], (((1,), (1,)), ((), ())), preferred_element_type=F32
            )
        for k in range(i):
            term = cot(k, i) * proj_f[k]
            total = term if total is None else total + term
        g, m = i // 2, i % 2
        gath[m][g, 0, 0, z, :samples, :] = total.astype(BF)
        gath[m][g, 0, 0, z, samples:, :] = meta[i].astype(BF)
        if i == 0:
            pl.semaphore_wait(barrier, nz - 1 + plane - 1)

        @pl.when(z < nz - 1)
        def _():
            z_up(g, m, z).start()

        @pl.when(z > 0)
        def _():
            z_down(g, m, z).start()

        spread(g, m, z)

    for d in range(1, plane):
        w1_copy(d).start()

    def z_stage(g, m):
        for t in range(1, nz):
            @pl.when(z - t >= 0)
            def _():
                z_up(g, m, z - t).wait_recv()

                @pl.when(z < nz - 1)
                def _():
                    z_up(g, m, z - t).start()

                spread(g, m, z - t)

            @pl.when(z + t < nz)
            def _():
                z_down(g, m, z + t).wait_recv()

                @pl.when(z > 0)
                def _():
                    z_down(g, m, z + t).start()

                spread(g, m, z + t)

    def a_stage(g, m):
        for o in range(1, wide[m]):
            for s in range(nz):
                a_copy(g, m, o, s).wait_recv()
                s_copy(g, m, o, s).start()

    def s_wait(g, m):
        for o in range(wide[m]):
            for s in range(nz):
                s_copy(g, m, o, s).wait_recv()

    row_number = lax.broadcasted_iota(jnp.int32, (rows, samples), 0).astype(F32).astype(BF)
    one, zero = jnp.ones((), BF), jnp.zeros((), BF)

    def sums_for(g, m, o):
        gx_to, gy_to = far[m](o)
        owner = (gx_to * size_gy + gy_to).astype(F32)
        blocks, values = [], []
        for core in range(2):
            for a in range(wide[m]):
                for s in range(nz):
                    note = gath[m][g, core, a, s, samples:, :].astype(F32)
                    key = jnp.where(note[:bag] == owner, note[bag:], -1.0).astype(BF)
                    count = None
                    for k in range(bag):
                        hit = jnp.where(row_number == key[k : k + 1, :], one, zero)
                        count = hit if count is None else count + hit
                    blocks.append(count)
                    values.append(gath[m][g, core, a, s, :samples, :])
        return jnp.dot(
            jnp.concatenate(blocks, axis=1),
            jnp.concatenate(values, axis=0),
            preferred_element_type=F32,
        )

    def weights_in_plane():
        total = w0[seat].astype(F32)
        for d in range(1, plane):
            w1_copy(d).wait_recv()
            total = total + w1[d].astype(F32)
        w2s[...] = total
        w2[z] = total
        for d in range(1, nz):
            w2_copy(d, z).start()

    def weights_along_z():
        for d in range(1, nz):
            w2_copy(d, (z + d) % nz).wait_recv()
        total = w2[0]
        for s in range(1, nz):
            total = total + w2[s]
        w3s[...] = total.astype(BF)
        w3[seat] = total.astype(BF)
        for d in range(1, plane):
            w3_copy(d, seat).start()

    def ahead(stage, g, m):
        if m == 0:
            stage(g, 1)
        else:
            @pl.when(g + 1 < fields // 2)
            def _():
                stage(g + 1, 0)

    z_stage(0, 0)
    a_stage(0, 0)

    def two_fields(g, carry):
        for m in range(2):
            ahead(z_stage, g, m)
            s_wait(g, m)

            def one_target(o, inner):
                part[m][o, g] = sums_for(g, m, o).astype(BF)
                p_copy(g, m, o).start()
                return inner

            lax.fori_loop(1, deep[m], one_target, 0)
            ahead(a_stage, g, m)
            out_ref[pl.ds(2 * g + m, rows, stride=fields), :] = sums_for(g, m, 0)

        @pl.when(g == 0)
        def _():
            weights_in_plane()

        @pl.when(g == 1)
        def _():
            weights_along_z()

        return carry

    lax.fori_loop(0, fields // 2, two_fields, 0)

    for d in range(1, plane):
        w3_copy(d, (seat + d) % plane).wait_recv()
    wout_ref[...] = w3[...].astype(F32)

    def finish(g, carry):
        for m in range(2):
            at = pl.ds(2 * g + m, rows, stride=fields)
            total = out_ref[at, :]
            for o in range(1, deep[m]):
                p_copy(g, m, o).wait_recv()
                total = total + got[m][o, g].astype(F32)
            out_ref[at, :] = total
        return carry

    lax.fori_loop(0, fields // 2, finish, 0)

    def drain(g, carry):
        for m in range(2):
            for s in range(nz):
                @pl.when((z >= s) & (z < nz - 1))
                def _():
                    z_up(g, m, s).wait_send()

                @pl.when((z <= s) & (z > 0))
                def _():
                    z_down(g, m, s).wait_send()

                for o in range(wide[m]):
                    if o:
                        a_copy(g, m, o, s).wait_send()
                    s_copy(g, m, o, s).wait_send()
            for o in range(1, deep[m]):
                p_copy(g, m, o).wait_send()
        return carry

    lax.fori_loop(0, fields // 2, drain, 0)
    for d in range(1, nz):
        w2_copy(d, z).wait_send()
    for d in range(1, plane):
        w1_copy(d).wait_send()
        w3_copy(d, seat).wait_send()


def on_device(size_gx, size_gy, pooled, cotangent, bilinear, bag_ids, bag_lens, row_home):
    samples, fields, width = pooled.shape
    bag = bag_ids.shape[2]
    rows = row_home.shape[1] // (size_gx * size_gy)
    nz, ny, plane = size_gx // 2, size_gy // 2, 2 * size_gy
    most, half = max(2, ny), fields // 2
    piece = (fields - 1) * width // plane
    vmem = pl.BlockSpec(memory_space=pltpu.VMEM)
    dma = pltpu.SemaphoreType.DMA
    table, weight = pl.pallas_call(
        functools.partial(kernel, size_gx, size_gy),
        out_shape=(
            jax.ShapeDtypeStruct((rows * fields, width), F32),
            jax.ShapeDtypeStruct((plane, piece, width), F32),
        ),
        in_specs=[vmem] * 6,
        out_specs=(vmem,) * 2,
        scratch_shapes=[
            pltpu.VMEM((samples * fields, width), F32),
            pltpu.VMEM((fields - 1, samples, width), F32),
            pltpu.VMEM((fields, 2 * bag, samples), F32),
            pltpu.VMEM((half, 2, 2, nz, samples + 2 * bag, width), BF),
            pltpu.VMEM((half, 2, ny, nz, samples + 2 * bag, width), BF),
            pltpu.VMEM((ny, half, rows, width), BF),
            pltpu.VMEM((2, half, rows, width), BF),
            pltpu.VMEM((ny, half, rows, width), BF),
            pltpu.VMEM((2, half, rows, width), BF),
            pltpu.VMEM((plane, piece, width), BF),
            pltpu.VMEM((plane, piece, width), BF),
            pltpu.VMEM((nz, piece, width), F32),
            pltpu.VMEM((piece, width), F32),
            pltpu.VMEM((plane, piece, width), BF),
            pltpu.VMEM((piece, width), BF),
            dma((fields * nz,)),
            dma((fields * nz,)),
            dma((fields * nz,)),
            dma((fields * most * nz,)),
            dma((fields * most * nz,)),
            dma((fields * most * nz,)),
            dma((fields * most * nz,)),
            dma((fields * most,)),
            dma((fields * most,)),
            dma((plane,)),
            dma((plane,)),
            dma((nz,)),
            dma((nz,)),
            dma((plane,)),
            dma((plane,)),
        ],
        compiler_params=pltpu.CompilerParams(collective_id=0, has_side_effects=True),
    )(
        pooled, cotangent.transpose(1, 0, 2), bilinear,
        bag_ids.transpose(1, 2, 0), bag_lens.transpose(1, 0), row_home,
    )
    return (
        weight.reshape(fields - 1, width, width),
        table.reshape(rows, fields, width),
    )


def solution(mesh):
    placed = (
        P(("gx", "gy"), None, None),
        P(("gx", "gy"), None, None),
        P(),
        P(("gx", "gy"), None, None),
        P(("gx", "gy"), None),
        P(),
    )
    return jax.shard_map(
        functools.partial(on_device, mesh.shape["gx"], mesh.shape["gy"]),
        mesh=mesh,
        in_specs=placed,
        out_specs=(P(), P(("gx", "gy"), None, None)),
        check_vma=False,
    )
```

```python
import functools

import jax
import jax.numpy as jnp
from jax import lax
from jax.experimental import pallas as pl
from jax.experimental.pallas import tpu as pltpu
from jax.sharding import PartitionSpec as P

MESH = pl.DeviceIdType.MESH
BF = jnp.bfloat16
F32 = jnp.float32
LANES = 128


def pair_list(fields):
    return [(i, j) for i in range(fields) for j in range(i + 1, fields)]


def kernel(
    size_gx, size_gy,
    pooled_ref, cot_ref, bil_ref, bag_ref, lens_ref, home_ref,
    out_ref, wout_ref,
    pool_f, proj_f, meta,
    gath, part, got,
    w0, w1, w2, w2s, w3, w3s,
    zs, zr, ss, sr, ps, pr,
    w1s_sem, w1r_sem, w2s_sem, w2r_sem, w3s_sem, w3r_sem,
):
    samples, fields, width = pooled_ref.shape
    bag = bag_ref.shape[1]
    rows = part.shape[2]
    piece = w0.shape[1]
    nz, ny = size_gx // 2, size_gy // 2
    plane = 2 * size_gy
    npc = 2 * ny
    gx, gy = lax.axis_index("gx"), lax.axis_index("gy")
    z, x, y, c = gx // 2, gx % 2, gy // 2, gy % 2
    spot = x * ny + y
    seat = x * size_gy + gy
    sibling = (gx, y * 2 + 1 - c)

    def spot_peer(d):
        to = (spot + d) % npc
        return (z * 2 + to // ny, (to % ny) * 2 + c)

    def z_peer(d):
        return (((z + d) % nz) * 2 + x, gy)

    def seat_peer(d):
        to = (seat + d) % plane
        return (z * 2 + to // size_gy, to % size_gy)

    def remote(src, dst, send, recv, dev):
        return pltpu.make_async_remote_copy(
            src_ref=src, dst_ref=dst, send_sem=send, recv_sem=recv,
            device_id=dev, device_id_type=MESH,
        )

    def z_copy(f, d):
        i = f * nz + d
        return remote(gath.at[f, 0, 0], gath.at[f, 0, d], zs.at[i], zr.at[i], z_peer(d))

    def s_copy(f, d):
        i = f * nz + d
        return remote(gath.at[f, 0, d], gath.at[f, 1, d], ss.at[i], sr.at[i], sibling)

    def p_copy(f, d):
        i = f * npc + d
        return remote(part.at[d, f], got.at[d, f], ps.at[i], pr.at[i], spot_peer(d))

    def w1_copy(d):
        return remote(
            w0.at[(seat + d) % plane], w1.at[d], w1s_sem.at[d], w1r_sem.at[d], seat_peer(d)
        )

    def w2_copy(d, slot):
        return remote(w2s, w2.at[slot], w2s_sem.at[d], w2r_sem.at[slot], z_peer(d))

    def w3_copy(d, slot):
        return remote(w3s, w3.at[slot], w3s_sem.at[d], w3r_sem.at[slot], seat_peer(d))

    barrier = pltpu.get_barrier_semaphore()
    for d in range(1, nz):
        pl.semaphore_signal(barrier, inc=1, device_id=z_peer(d), device_id_type=MESH)
    for d in range(1, plane):
        pl.semaphore_signal(barrier, inc=1, device_id=seat_peer(d), device_id_type=MESH)

    def spread_out(b, carry):
        pool_f[pl.ds(pl.multiple_of(b * fields, fields), fields), :] = pooled_ref[b].astype(F32)
        return carry

    lax.fori_loop(0, samples, spread_out, 0, unroll=8)

    bags = [bag_ref[:, k, :] for k in range(bag)]
    high = [b // LANES for b in bags]
    low = [b % LANES for b in bags]

    def look(h, found):
        row = home_ref[:, pl.ds(pl.multiple_of(h * LANES, LANES), LANES)]
        return tuple(
            jnp.where(high[k] == h, jnp.take_along_axis(row, low[k], axis=1), found[k])
            for k in range(bag)
        )

    none = jnp.full(lens_ref.shape, 0, jnp.int32)
    found = lax.fori_loop(0, home_ref.shape[1] // LANES, look, (none,) * bag, unroll=8)
    lens = lens_ref[...]
    for k in range(bag):
        meta[:, k, :] = jnp.where(lens > k, found[k] // rows, -1).astype(F32)
        meta[:, bag + k, :] = (found[k] % rows).astype(F32)

    pool = lambda f: pool_f[pl.ds(f, samples, stride=fields), :]
    number = {pair: p for p, pair in enumerate(pair_list(fields))}
    cot = lambda i, j: cot_ref[number[i, j]].astype(F32)

    for i in range(fields):
        total = None
        if i < fields - 1:
            mine = pool(i).astype(BF)
            proj_f[i] = jnp.dot(mine, bil_ref[i], preferred_element_type=F32)
            upper = jnp.zeros((samples, width), F32)
            for j in range(i + 1, fields):
                upper = upper + cot(i, j) * pool(j)
            upper = upper.astype(BF)
            wide_w = lax.dot_general(
                mine, upper, (((0,), (0,)), ((), ())), preferred_element_type=F32
            ).astype(BF)
            at, end = i * width, (i + 1) * width
            while at < end:
                p, r = at // piece, at % piece
                n = min(piece - r, end - at)
                w0[p, r : r + n, :] = wide_w[at - i * width : at - i * width + n, :]
                at += n
            total = lax.dot_general(
                upper, bil_ref[i], (((1,), (1,)), ((), ())), preferred_element_type=F32
            )
        for k in range(i):
            term = cot(k, i) * proj_f[k]
            total = term if total is None else total + term
        gath[i, 0, 0, :samples, :] = total.astype(BF)
        gath[i, 0, 0, samples:, :] = meta[i].astype(BF)
        if i == 0:
            pl.semaphore_wait(barrier, nz - 1 + plane - 1)

        for d in range(1, nz):
            z_copy(i, d).start()
        s_copy(i, 0).start()

    for d in range(1, plane):
        w1_copy(d).start()

    def forward(f):
        for d in range(1, nz):
            z_copy(f, d).wait_recv()
            s_copy(f, d).start()

    row_number = lax.broadcasted_iota(jnp.int32, (rows, samples), 0).astype(F32).astype(BF)
    one, zero = jnp.ones((), BF), jnp.zeros((), BF)

    def sums_for(f, d):
        gx_to, gy_to = spot_peer(d)
        owner = (gx_to * size_gy + gy_to).astype(F32)
        blocks, values = [], []
        for core in range(2):
            for s in range(nz):
                note = gath[f, core, s, samples:, :].astype(F32)
                key = jnp.where(note[:bag] == owner, note[bag:], -1.0).astype(BF)
                count = None
                for k in range(bag):
                    hit = jnp.where(row_number == key[k : k + 1, :], one, zero)
                    count = hit if count is None else count + hit
                blocks.append(count)
                values.append(gath[f, core, s, :samples, :])
        return jnp.dot(
            jnp.concatenate(blocks, axis=1),
            jnp.concatenate(values, axis=0),
            preferred_element_type=F32,
        )

    def weights_in_plane():
        total = w0[seat].astype(F32)
        for d in range(1, plane):
            w1_copy(d).wait_recv()
            total = total + w1[d].astype(F32)
        w2s[...] = total
        w2[z] = total
        for d in range(1, nz):
            w2_copy(d, z).start()

    def weights_along_z():
        for d in range(1, nz):
            w2_copy(d, (z + d) % nz).wait_recv()
        total = w2[0]
        for s in range(1, nz):
            total = total + w2[s]
        w3s[...] = total.astype(BF)
        w3[seat] = total.astype(BF)
        for d in range(1, plane):
            w3_copy(d, seat).start()

    forward(0)

    def one_field(f, carry):
        @pl.when(f + 1 < fields)
        def _():
            forward(f + 1)

        for d in range(nz):
            s_copy(f, d).wait_recv()

        def one_target(d, inner):
            part[d, f] = sums_for(f, d).astype(BF)
            p_copy(f, d).start()
            return inner

        lax.fori_loop(1, npc, one_target, 0)
        out_ref[pl.ds(f, rows, stride=fields), :] = sums_for(f, 0)

        @pl.when(f == 1)
        def _():
            weights_in_plane()

        @pl.when(f == 3)
        def _():
            weights_along_z()

        return carry

    lax.fori_loop(0, fields, one_field, 0)

    for d in range(1, plane):
        w3_copy(d, (seat + d) % plane).wait_recv()
    wout_ref[...] = w3[...].astype(F32)

    def finish(f, carry):
        at = pl.ds(f, rows, stride=fields)
        total = out_ref[at, :]
        for d in range(1, npc):
            p_copy(f, d).wait_recv()
            total = total + got[d, f].astype(F32)
        out_ref[at, :] = total
        return carry

    lax.fori_loop(0, fields, finish, 0)

    def drain(f, carry):
        for d in range(1, nz):
            z_copy(f, d).wait_send()
        for d in range(nz):
            s_copy(f, d).wait_send()
        for d in range(1, npc):
            p_copy(f, d).wait_send()
        return carry

    lax.fori_loop(0, fields, drain, 0)
    for d in range(1, nz):
        w2_copy(d, z).wait_send()
    for d in range(1, plane):
        w1_copy(d).wait_send()
        w3_copy(d, seat).wait_send()


def on_device(size_gx, size_gy, pooled, cotangent, bilinear, bag_ids, bag_lens, row_home):
    samples, fields, width = pooled.shape
    bag = bag_ids.shape[2]
    rows = row_home.shape[1] // (size_gx * size_gy)
    nz, ny, plane = size_gx // 2, size_gy // 2, 2 * size_gy
    npc = 2 * ny
    piece = (fields - 1) * width // plane
    vmem = pl.BlockSpec(memory_space=pltpu.VMEM)
    dma = pltpu.SemaphoreType.DMA
    table, weight = pl.pallas_call(
        functools.partial(kernel, size_gx, size_gy),
        out_shape=(
            jax.ShapeDtypeStruct((rows * fields, width), F32),
            jax.ShapeDtypeStruct((plane, piece, width), F32),
        ),
        in_specs=[vmem] * 6,
        out_specs=(vmem,) * 2,
        scratch_shapes=[
            pltpu.VMEM((samples * fields, width), F32),
            pltpu.VMEM((fields - 1, samples, width), F32),
            pltpu.VMEM((fields, 2 * bag, samples), F32),
            pltpu.VMEM((fields, 2, nz, samples + 2 * bag, width), BF),
            pltpu.VMEM((npc, fields, rows, width), BF),
            pltpu.VMEM((npc, fields, rows, width), BF),
            pltpu.VMEM((plane, piece, width), BF),
            pltpu.VMEM((plane, piece, width), BF),
            pltpu.VMEM((nz, piece, width), F32),
            pltpu.VMEM((piece, width), F32),
            pltpu.VMEM((plane, piece, width), BF),
            pltpu.VMEM((piece, width), BF),
            dma((fields * nz,)),
            dma((fields * nz,)),
            dma((fields * nz,)),
            dma((fields * nz,)),
            dma((fields * npc,)),
            dma((fields * npc,)),
            dma((plane,)),
            dma((plane,)),
            dma((nz,)),
            dma((nz,)),
            dma((plane,)),
            dma((plane,)),
        ],
        compiler_params=pltpu.CompilerParams(collective_id=0, has_side_effects=True),
    )(
        pooled, cotangent.transpose(1, 0, 2), bilinear,
        bag_ids.transpose(1, 2, 0), bag_lens.transpose(1, 0), row_home,
    )
    return (
        weight.reshape(fields - 1, width, width),
        table.reshape(rows, fields, width),
    )


def solution(mesh):
    placed = (
        P(("gx", "gy"), None, None),
        P(("gx", "gy"), None, None),
        P(),
        P(("gx", "gy"), None, None),
        P(("gx", "gy"), None),
        P(),
    )
    return jax.shard_map(
        functools.partial(on_device, mesh.shape["gx"], mesh.shape["gy"]),
        mesh=mesh,
        in_specs=placed,
        out_specs=(P(), P(("gx", "gy"), None, None)),
        check_vma=False,
    )
```
